256 devices in a mesh: ep: 8 (over z), tp: 32 (over y, x, core).
Axes of the slice: x: 4, y: 4, z: 8, core: 2. Of those that a mesh axis runs over, the one named last changes fastest.
Arguments:
- tokens: bfloat16 [768, 3072], P('ep', 'tp'), may hold values from -6 to 6
- cotangent: bfloat16 [768, 3072], P('ep', 'tp'), may hold values from -6 to 6
- expert_ids: int32 [768, 2], P('ep'), may hold values from 0 to 7, all different within a row; in each aligned block of 96 rows (0 to 95, 96 to 191, ...) at most 40 rows name the same one
- combine_weights: float32 [768, 2], P('ep'), may hold values from 0.1 to 1
- w_gate: bfloat16 [8, 3072, 8192], P('ep', None, 'tp'), may hold values from -0.21875 to 0.21875
- w_up: bfloat16 [8, 3072, 8192], P('ep', None, 'tp'), may hold values from -0.109375 to 0.109375
- w_down: bfloat16 [8, 8192, 3072], P('ep', 'tp'), may hold values from -0.125 to 0.125
Outputs:
- mixed: bfloat16 [768, 3072], P('ep', 'tp')
- grad_tokens: bfloat16 [768, 3072], P('ep', 'tp')
- grad_combine: float32 [768, 2], P('ep')
- grad_gate: bfloat16 [8, 3072, 8192], P('ep', 'tp')
- grad_up: bfloat16 [8, 3072, 8192], P('ep', 'tp')
- grad_down: bfloat16 [8, 8192, 3072], P('ep', None, 'tp')
The draws below stay inside these ranges and needn't reach their ends.
Inputs may be any that keep to these rules, and one draw needn't show every extreme that they name: `expert_ids`: each row names 2 different experts. Among the 96 rows of one index of ep, no expert is named more than 40 times, and in some such blocks one expert is named exactly 40 times.
All inputs are finite; a program needn't handle non-finite values.
Results may differ from the reference program's by a relative error of at most 0.019.
Values may be sent and summed in bfloat16 or wider, within the bound.
No kernel may reach another device: no remote copies, remote signals or barrier semaphores. Data moves between devices by JAX's collectives and lax.ppermute only.
A program may use at most 64 MiB of HBM per device.

```python
import math
import jax
import jax.numpy as jnp
import numpy as np
from jax import lax

D = 3072
FF = 8192
TOP = 2
TOK_EP = 96
EXPERTS = 8
CAP = 40
TOKENS = 768
N_EP = 8
N_TP = 32


def with_spikes(drawn, stream_key, source, target, parts, factor):
    def block_of(axis_at):
        return (jnp.arange(drawn.shape[axis_at]) // (drawn.shape[axis_at] // parts)).reshape((-1,) + (1,) * (drawn.ndim - 1 - axis_at))

    first = jax.random.permutation(stream_key, parts)[block_of(target)]
    other_side = (block_of(target) + parts // 2) % parts
    return jnp.where((block_of(source) == first) | (block_of(source) == other_side), factor * drawn, drawn)


def level_of(stream_key, shape, shards, least, largest):
    def one(position, parts):
        draws = jax.random.uniform(jax.random.fold_in(jax.random.fold_in(stream_key, 6), position), (parts,), jnp.float32, least / len(shards), largest / len(shards))
        return jnp.repeat(jnp.exp(draws), shape[position] // parts).reshape((-1,) + (1,) * (len(shape) - position - 1))

    loudness = one(*shards[0])
    for cut in shards[1:]:
        loudness = loudness * one(*cut)
    return loudness


def assign_block(key, own, number, rows, amount, top, most, skew):
    ranking = jax.random.permutation(key, amount)
    packed, usual = shares(amount, rows * top, most, skew, True), shares(amount, rows * top, most, skew, False)
    places = jnp.arange(amount)

    def named(tallies, rotation):
        used = int((tallies > 0).sum())
        fixed = max(1, used // 4)
        passed = fixed + (places - fixed + rotation * (used - fixed)) % max(1, amount - fixed)
        return jnp.zeros((amount,), jnp.int32).at[ranking[jnp.where(places < fixed, places, passed)]].set(jnp.asarray(tallies, jnp.int32))

    tallies = jnp.where(number % 4 == 0, named(packed, number // 4), named(usual, number - number // 4 - 1))
    mixed = jax.random.permutation(jax.random.fold_in(own, 3), amount)
    giver, receiver = mixed[0:amount // 2 * 2:2], mixed[1:amount // 2 * 2:2]
    margin = jnp.minimum(tallies[giver] - 1, most - tallies[receiver]) // 2
    margin = jnp.where((giver == ranking[0]) | (receiver == ranking[0]) | (tallies[receiver] == 0), 0, jnp.maximum(margin, 0))
    passed = jax.random.randint(jax.random.fold_in(own, 4), (amount // 2,), 0, 1 << 20) % (margin + 1)
    tallies = tallies.at[giver].add(-passed).at[receiver].add(passed)
    members = jnp.searchsorted(jnp.cumsum(tallies), jnp.arange(rows * top), side="right").astype(jnp.int32)
    grid = members.reshape(top, rows).T
    grid = grid[jax.random.permutation(jax.random.fold_in(own, 1), rows)]
    rotation = jax.random.randint(jax.random.fold_in(own, 2), (rows, 1), 0, top)
    return jnp.take_along_axis(grid, (jnp.arange(top)[None, :] + rotation) % top, axis=1)


def shares(count, total, bound, lean, full):
    portions = [(1 << 20) // math.isqrt(standing ** lean) + 1 for standing in range(1, count + 1)]
    largest = bound if full else min(bound, max(-(-total // count), total * portions[0] // sum(portions)))
    least = 1 if total - largest >= count - 1 else 0
    given, spare = [largest] + [least] * (count - 1), total - largest - least * (count - 1)
    while spare > 0:
        candidates = [i for i in range(1, count) if given[i] < largest] or [i for i in range(1, count) if given[i] < bound]
        mass, left = sum([portions[i] for i in candidates]), spare
        for i in candidates:
            extra = min(bound - given[i], max(1, left * portions[i] // mass), spare)
            given[i] = given[i] + extra
            spare = spare - extra
    return np.array(given)


def noise(key, extent, scale, limit, cuts=(), held_as=jnp.bfloat16):
    result = scale * jax.random.normal(key, extent, jnp.float32)
    if cuts:
        result = result * level_of(key, extent, cuts, -0.22, 0.18)
    return jnp.clip(result, -limit, limit).astype(held_as)


def heavy_noise(own_key, dims, spread, bound, shards, heavy, kind=jnp.bfloat16):
    values = spread * jax.random.normal(own_key, dims, jnp.float32)
    if shards:
        values = values * level_of(own_key, dims, shards, -0.22, 0.18)
    return jnp.clip(with_spikes(values, jax.random.fold_in(own_key, 3), *heavy), -bound, bound).astype(kind)


def setup_inputs(seed: int = 0) -> dict:
    key_of = jax.random.split(jax.random.key(seed), 8)
    tokens = noise(key_of[0], (TOKENS, D), 1.0, 6.0, ((0, 8), (1, 32)))
    cotangent = noise(key_of[1], (TOKENS, D), 1.0, 6.0, ((0, 8), (1, 32)))
    expert_ids_keys = jax.random.split(jax.random.fold_in(key_of[2], 1), TOKENS // TOK_EP)
    expert_ids_turns = jax.random.permutation(jax.random.fold_in(key_of[2], 3), TOKENS // TOK_EP)
    expert_ids = jax.vmap(lambda own, number: assign_block(jax.random.fold_in(key_of[2], 2), own, number, TOK_EP, N_EP, TOP, CAP, 2))(expert_ids_keys, expert_ids_turns).reshape((TOKENS, TOP))
    combine_weights = jnp.clip(jnp.exp(math.log(1.0) - 2.3025851 * jax.random.uniform(key_of[3], (TOKENS, TOP), jnp.float32) ** level_of(key_of[3], (TOKENS, TOP), ((0, 8),), -0.2, 0.2)), 0.1, 1.0)
    w_gate = heavy_noise(key_of[4], (EXPERTS, D, FF), D ** -0.5, 0.21875, ((0, 8), (2, 32)), (2, 1, 32, 2.75))
    w_up = noise(key_of[5], (EXPERTS, D, FF), D ** -0.5, 0.109375, ((0, 8), (2, 32)))
    w_down = heavy_noise(key_of[6], (EXPERTS, FF, D), FF ** -0.5, 0.125, ((0, 8), (1, 32)), (1, 2, 32, 2.75))
    return {"tokens": tokens, "cotangent": cotangent, "expert_ids": expert_ids, "combine_weights": combine_weights, "w_gate": w_gate, "w_up": w_up, "w_down": w_down}


def silu_parts(gate_pre):
    sigma = jax.nn.sigmoid(gate_pre)
    return gate_pre * sigma, sigma * (1.0 + gate_pre * (1.0 - sigma))


def slot_rows(expert_ids):
    groups = expert_ids.reshape(N_EP, TOK_EP * TOP)
    onehot = (groups[:, :, None] == jnp.arange(N_EP, dtype=jnp.int32)[None, None, :]).astype(jnp.int32)
    before = jnp.cumsum(onehot, axis=1) - onehot
    rank = jnp.sum(before * onehot, axis=2)
    source = jnp.arange(N_EP, dtype=jnp.int32)[:, None]
    return (source * CAP + rank).reshape(-1).astype(jnp.int32)


def rounded_blocks(pairs, rows):
    width = FF // N_TP

    def step(total, index):
        start = index * width
        part = jnp.zeros((rows, D), jnp.float32)
        for left, right in pairs:
            left_block = lax.dynamic_slice_in_dim(left, start, width, 1)
            right_block = lax.dynamic_slice_in_dim(right, start, width, 0)
            part = part + jnp.dot(left_block, right_block, preferred_element_type=jnp.float32)
        rounded = lax.optimization_barrier(part.astype(jnp.bfloat16))
        return total + rounded.astype(jnp.float32), None

    total, _ = lax.scan(step, jnp.zeros((rows, D), jnp.float32), jnp.arange(N_TP, dtype=jnp.int32))
    return total.astype(jnp.bfloat16)


def reference(tokens, cotangent, expert_ids, combine_weights, w_gate, w_up, w_down):
    flat_ids = expert_ids.reshape(-1)
    rows = slot_rows(expert_ids)
    owner = jnp.repeat(jnp.arange(TOKENS, dtype=jnp.int32), TOP)
    weight_flat = combine_weights.reshape(-1)
    buffer_rows = N_EP * CAP
    x_buffer = jnp.zeros((N_EP, buffer_rows, D), jnp.bfloat16).at[flat_ids, rows].set(tokens[owner])
    grad_out = (weight_flat[:, None] * cotangent[owner].astype(jnp.float32)).astype(jnp.bfloat16)
    dy_buffer = jnp.zeros((N_EP, buffer_rows, D), jnp.bfloat16).at[flat_ids, rows].set(grad_out)
    outs_list, ins_list, gates_list, ups_list, downs_list = [], [], [], [], []
    for expert in range(N_EP):
        x_rows = x_buffer[expert]
        dy_rows = dy_buffer[expert]
        gate_pre = jnp.dot(x_rows, w_gate[expert], preferred_element_type=jnp.float32)
        up_pre = jnp.dot(x_rows, w_up[expert], preferred_element_type=jnp.float32)
        active, slope = silu_parts(gate_pre)
        hidden = (active * up_pre).astype(jnp.bfloat16)
        outs_list.append(rounded_blocks([(hidden, w_down[expert])], buffer_rows))
        grad_hidden = jnp.dot(dy_rows, w_down[expert].T, preferred_element_type=jnp.float32)
        grad_gate_pre = (grad_hidden * up_pre * slope).astype(jnp.bfloat16)
        grad_up_pre = (grad_hidden * active).astype(jnp.bfloat16)
        ins_list.append(rounded_blocks([(grad_gate_pre, w_gate[expert].T), (grad_up_pre, w_up[expert].T)], buffer_rows))
        gates_list.append(jnp.dot(x_rows.T, grad_gate_pre, preferred_element_type=jnp.float32).astype(jnp.bfloat16))
        ups_list.append(jnp.dot(x_rows.T, grad_up_pre, preferred_element_type=jnp.float32).astype(jnp.bfloat16))
        downs_list.append(jnp.dot(hidden.T, dy_rows, preferred_element_type=jnp.float32).astype(jnp.bfloat16))
    expert_out = jnp.stack(outs_list)[flat_ids, rows].reshape(TOKENS, TOP, D).astype(jnp.float32)
    grad_in = jnp.stack(ins_list)[flat_ids, rows].reshape(TOKENS, TOP, D).astype(jnp.float32)
    mixed = jnp.sum(combine_weights[:, :, None] * expert_out, axis=1).astype(jnp.bfloat16)
    grad_combine = jnp.sum(cotangent.astype(jnp.float32)[:, None, :] * expert_out, axis=2)
    grad_tokens = jnp.sum(grad_in, axis=1).astype(jnp.bfloat16)
    return (mixed, grad_tokens, grad_combine, jnp.stack(gates_list), jnp.stack(ups_list), jnp.stack(downs_list))
```

```python
import jax
import jax.numpy as jnp
from jax import lax
from jax.experimental import pallas as pl
from jax.experimental.pallas import tpu as pltpu
from jax.sharding import PartitionSpec as P

BF = jnp.bfloat16
F32 = jnp.float32


def dot(a, b, ca, cb):
    return lax.dot_general(a, b, (((ca,), (cb,)), ((), ())), preferred_element_type=F32)


def halves(v):
    hi = v.astype(BF)
    return hi, (v - hi.astype(F32)).astype(BF)


def lay_out(pieces):
    n, rows, total = pieces.shape
    width = total // 3

    def kernel(src, *refs):
        outs, sems = refs[:3], refs[3]
        copies = []
        for m in range(3):
            for s in range(n):
                copies.append(
                    pltpu.make_async_copy(
                        src.at[s, :, pl.ds(m * width, width)],
                        outs[m].at[:, pl.ds(s * width, width)],
                        sems.at[m * n + s],
                    )
                )
        for c in copies:
            c.start()
        for c in copies:
            c.wait()

    return pl.pallas_call(
        kernel,
        out_shape=[jax.ShapeDtypeStruct((rows, n * width), pieces.dtype)] * 3,
        in_specs=[pl.BlockSpec(memory_space=pl.ANY)],
        out_specs=[pl.BlockSpec(memory_space=pl.ANY)] * 3,
        scratch_shapes=[pltpu.SemaphoreType.DMA((3 * n,))],
        name="lay_out",
    )(pieces)


def body(tokens, cotangent, expert_ids, combine_weights, w_gate, w_up, w_down):
    groups = lax.axis_size("ep")
    devices = lax.axis_size("tp")
    chips = devices // 2
    tok_rows, width = tokens.shape
    chosen = expert_ids.shape[1]
    cap = tok_rows * chosen * 5 // (3 * groups)
    rows = groups * cap
    wg, wu, wd = w_gate[0], w_up[0], w_down[0]
    hid = wg.shape[1]
    feats = wg.shape[0]
    core = lax.axis_index("tp") % 2
    same_core = [[2 * i + c for i in range(chips)] for c in range(2)]
    swap = [(i, i ^ 1) for i in range(devices)]

    ids = [expert_ids[:, k] for k in range(chosen)]
    hot = [
        (i[:, None] == jnp.arange(groups, dtype=jnp.int32)[None, :]).astype(F32) for i in ids
    ]
    both = sum(hot)
    t = jnp.arange(tok_rows, dtype=jnp.int32)
    before = jnp.dot((t[:, None] > t[None, :]).astype(F32), both)
    place = []
    for k in range(chosen):
        rank = jnp.sum(before * hot[k], axis=1).astype(jnp.int32)
        slot = ids[k] * cap + rank
        place.append((slot[None, :] == jnp.arange(rows, dtype=jnp.int32)[:, None]).astype(BF))
    cot = cotangent.astype(F32)
    weight = [combine_weights[:, k][:, None] for k in range(chosen)]
    send_rows = dot(sum(place), tokens, 1, 0)
    send_grad = sum(dot(place[k], (weight[k] * cot).astype(BF), 1, 0) for k in range(chosen))
    send = jnp.concatenate(
        [send_rows.reshape(groups, cap, width), send_grad.reshape(groups, cap, width)], axis=1
    ).astype(BF)
    recv = lax.all_to_all(send, "ep", 0, 0, tiled=True)
    piece = (
        jnp.concatenate(
            [recv[:, :cap].reshape(rows, width), recv[:, cap:].reshape(rows, width)], axis=0
        )
    ).T

    mine = lax.all_to_all(
        jnp.broadcast_to(piece[None], (chips, *piece.shape)),
        "tp", 0, 0, tiled=True, axis_index_groups=same_core,
    )
    theirs = lax.ppermute(mine, "tp", swap)
    full = jnp.where(
        (jnp.arange(2) == core)[None, :, None, None], mine[:, None], theirs[:, None]
    ).reshape(feats, 2 * rows)
    x, dy = full[:, :rows], full[:, rows:]

    gate_pre = dot(x, wg, 0, 0)
    up_pre = dot(x, wu, 0, 0)
    sigma = jax.nn.sigmoid(gate_pre)
    active = gate_pre * sigma
    slope = sigma * (1.0 + gate_pre * (1.0 - sigma))
    hidden = (active * up_pre).astype(BF)
    grad_hidden = dot(dy, wd, 0, 1)
    ggp = (grad_hidden * up_pre * slope).astype(BF)
    gup = (grad_hidden * active).astype(BF)
    inner = jnp.sum(hidden.astype(F32) * grad_hidden, axis=1)

    out_t = dot(wd, hidden, 0, 1)
    in_t = dot(wg, ggp, 1, 1) + dot(wu, gup, 1, 1)
    part = jnp.concatenate([out_t, in_t], axis=1).astype(BF).reshape(chips, 2, width, 2 * rows)
    keep = lax.dynamic_index_in_dim(part, core, 1, keepdims=False)
    give = lax.dynamic_index_in_dim(part, 1 - core, 1, keepdims=False)
    got = lax.ppermute(give, "tp", swap)
    inner = inner + lax.ppermute(inner, "tp", swap)
    hi, lo = halves(inner)
    extra = jnp.pad(jnp.stack([hi, lo]), ((0, 6), (0, rows)))
    reduced = (keep.astype(F32) + got.astype(F32)).astype(BF)
    reduced = jnp.concatenate(
        [reduced, jnp.broadcast_to(extra[None], (chips, 8, 2 * rows))], axis=1
    )
    summed = jnp.sum(
        lax.all_to_all(
            reduced, "tp", 0, 0, tiled=True, axis_index_groups=same_core
        ).astype(F32),
        axis=0,
    )

    both_grads = dot(x, jnp.concatenate([ggp, gup], axis=1), 1, 0).astype(BF)
    down_grad = dot(dy, hidden, 1, 0).astype(BF)
    grads = jnp.concatenate([both_grads, down_grad], axis=1).reshape(devices, width, 3 * hid)
    pieces = lax.all_to_all(grads, "tp", 0, 0, tiled=True)

    hi, lo = halves(summed[width] + summed[width + 1])
    back = jnp.concatenate(
        [summed[:width].astype(BF), hi[None], lo[None], jnp.zeros((6, 2 * rows), BF)], axis=0
    ).T.reshape(2, groups, cap, width + 8)
    back = jnp.concatenate([back[0], back[1]], axis=1)
    back = lax.all_to_all(back, "ep", 0, 0, tiled=True)
    out_back = back[:, :cap].reshape(rows, width + 8)
    in_back = back[:, cap:].reshape(rows, width + 8)
    chosen_out = [dot(place[k], out_back, 0, 0) for k in range(chosen)]
    mixed = sum(weight[k] * chosen_out[k][:, :width] for k in range(chosen)).astype(BF)
    grad_combine = jnp.concatenate(
        [
            (chosen_out[k][:, width : width + 1] + chosen_out[k][:, width + 1 : width + 2])
            / weight[k]
            for k in range(chosen)
        ],
        axis=1,
    )
    grad_tokens = dot(sum(place), in_back[:, :width], 0, 0).astype(BF)

    gate_out, up_out, down_out = lay_out(pieces)
    return (
        mixed,
        grad_tokens,
        grad_combine,
        gate_out[None],
        up_out[None],
        down_out.T[None],
    )


def solution(mesh):
    return jax.shard_map(
        body,
        mesh=mesh,
        in_specs=(
            P("ep", "tp"),
            P("ep", "tp"),
            P("ep", None),
            P("ep", None),
            P("ep", None, "tp"),
            P("ep", None, "tp"),
            P("ep", "tp", None),
        ),
        out_specs=(
            P("ep", "tp"),
            P("ep", "tp"),
            P("ep", None),
            P("ep", "tp", None),
            P("ep", "tp", None),
            P("ep", None, "tp"),
        ),
        check_vma=False,
    )
```

```python
import math

import jax
import jax.numpy as jnp
from jax import lax
from jax.experimental import pallas as pl
from jax.experimental.pallas import tpu as pltpu
from jax.sharding import PartitionSpec as P

BF = jnp.bfloat16
F32 = jnp.float32


def dot(a, b, ca, cb):
    return lax.dot_general(a, b, (((ca,), (cb,)), ((), ())), preferred_element_type=F32)


def halves(v):
    hi = v.astype(BF)
    return hi, (v - hi.astype(F32)).astype(BF)


def vmem():
    return pl.BlockSpec(memory_space=pltpu.VMEM)


def smem():
    return pl.BlockSpec(memory_space=pltpu.SMEM)


def partials(core, hidden, ggp, gup, wg, wu, wd, chips, width, steps=4):
    rows, hid = hidden.shape
    feats = wg.shape[0]
    block = feats // steps
    each = chips // steps
    lanes = 2 * rows
    pad = 64

    def kernel(core_ref, h_ref, g_ref, u_ref, wg_ref, wu_ref, wd_ref, keep_ref, give_ref, both):
        zeros = jnp.zeros((pad, hid), BF)
        h = jnp.concatenate([h_ref[...], zeros], axis=0)
        g = jnp.concatenate([zeros, g_ref[...]], axis=0)
        u = jnp.concatenate([zeros, u_ref[...]], axis=0)
        out_t = dot(wd_ref[...].T, h, 1, 1)
        in_t = dot(wg_ref[...], g, 1, 1) + dot(wu_ref[...], u, 1, 1)
        mid = rows - pad
        joined = jnp.concatenate(
            [
                out_t[:, :mid],
                out_t[:, mid : mid + 128] + in_t[:, :128],
                in_t[:, 128:],
            ],
            axis=1,
        ).astype(BF)
        both[...] = joined.reshape(each, 2, width, lanes)
        c = core_ref[0]
        for i in range(each):
            keep_ref[i] = both[i, c]
            give_ref[i] = both[i, 1 - c]

    whole = pl.BlockSpec((rows, hid), lambda i: (0, 0))
    out = pl.BlockSpec((each, width, lanes), lambda i: (i, 0, 0))
    return pl.pallas_call(
        kernel,
        grid=(steps,),
        out_shape=[jax.ShapeDtypeStruct((chips, width, lanes), BF)] * 2,
        in_specs=[
            smem(),
            whole,
            whole,
            whole,
            pl.BlockSpec((block, hid), lambda i: (i, 0)),
            pl.BlockSpec((block, hid), lambda i: (i, 0)),
            pl.BlockSpec((hid, block), lambda i: (0, i)),
        ],
        out_specs=[out, out],
        scratch_shapes=[pltpu.VMEM((each, 2, width, lanes), BF)],
        name="partials",
    )(core, hidden, ggp, gup, wg, wu, wd)


def add_pair(keep, got, extra, steps=2):
    chips, width, lanes = keep.shape
    more = extra.shape[0]
    each = chips // steps

    def kernel(a, b, e, o):
        o[:, :width] = (a[...].astype(F32) + b[...].astype(F32)).astype(BF)
        for i in range(each):
            o[i, width:] = e[...]

    spec = pl.BlockSpec((each, width, lanes), lambda i: (i, 0, 0))
    return pl.pallas_call(
        kernel,
        grid=(steps,),
        out_shape=jax.ShapeDtypeStruct((chips, width + more, lanes), BF),
        in_specs=[spec, spec, pl.BlockSpec((more, lanes), lambda i: (0, 0))],
        out_specs=pl.BlockSpec((each, width + more, lanes), lambda i: (i, 0, 0)),
        name="add_pair",
    )(keep, got, extra)


def weight_grads(blocks, mine, factors):
    chips, width, lanes = mine.shape
    rows = lanes // 2
    n = len(factors)
    side = blocks.shape[0]
    pad = 64
    deep = rows + pad

    def kernel(*refs):
        idx, src = refs[0], refs[1]
        fs, outs = refs[2 : 2 + n], refs[2 + n : 2 + n + side]
        lhs, g, h = refs[2 + n + side :]
        for j in range(side):
            lhs[j * width : (j + 1) * width] = src[idx[j]]
        g[rows:] = jnp.zeros((pad, n * 256), BF)
        h[:pad] = jnp.zeros((pad, n * 128), BF)
        for s in range(n):
            g[:rows, s * 256 : (s + 1) * 256] = fs[s][:, :256]
            h[pad:, s * 128 : (s + 1) * 128] = fs[s][:, 256:]
        for s in range(0, n, 2):
            rg = dot(lhs[:, :deep], g[:, s * 256 : (s + 2) * 256], 1, 0).astype(BF)
            rh = dot(lhs[:, lanes - deep :], h[:, s * 128 : (s + 2) * 128], 1, 0).astype(BF)
            for j in range(side):
                at = slice(j * width, (j + 1) * width)
                for i in range(2):
                    o = (s + i) * 384
                    outs[j][:, o : o + 256] = rg[at, i * 256 : (i + 1) * 256]
                    outs[j][:, o + 256 : o + 384] = rh[at, i * 128 : (i + 1) * 128]

    return pl.pallas_call(
        kernel,
        out_shape=[jax.ShapeDtypeStruct((width, n * 384), BF)] * side,
        in_specs=[smem()] + [vmem()] * (1 + n),
        out_specs=[vmem()] * side,
        scratch_shapes=[
            pltpu.VMEM((side * width, lanes), BF),
            pltpu.VMEM((deep, n * 256), BF),
            pltpu.VMEM((deep, n * 128), BF),
        ],
        name="weight_grads",
    )(blocks, mine, *factors)


def lay_out(columns, pieces, hid, steps=3):
    width, wide = pieces[0].shape
    n = len(pieces)
    per = wide // 384
    total = n * per * 128
    block = width // steps

    def kernel(cols, *refs):
        ins, outs = refs[:n], refs[n:]
        for p in range(n):
            for s in range(per):
                at = pl.multiple_of(cols[p * per + s], 128)
                for m in range(3):
                    o = (s * 3 + m) * 128
                    outs[m][:, pl.ds(at, 128)] = ins[p][:, o : o + 128]

    return pl.pallas_call(
        kernel,
        grid=(steps,),
        out_shape=[jax.ShapeDtypeStruct((width, total), BF)] * 3,
        in_specs=[smem()] + [pl.BlockSpec((block, wide), lambda i: (i, 0))] * n,
        out_specs=[pl.BlockSpec((block, total), lambda i: (i, 0))] * 3,
        name="lay_out",
    )(columns, *pieces)


def body(tokens, cotangent, expert_ids, combine_weights, w_gate, w_up, w_down):
    groups = lax.axis_size("ep")
    devices = lax.axis_size("tp")
    chips = devices // 2
    tok_rows, width = tokens.shape
    chosen = expert_ids.shape[1]
    cap = tok_rows * chosen * 5 // (3 * groups)
    rows = groups * cap
    wg, wu, wd = w_gate[0], w_up[0], w_down[0]
    hid = wg.shape[1]
    feats = wg.shape[0]
    side = math.isqrt(chips)
    here = lax.axis_index("tp")
    core, cx, cy = here % 2, here // 2 % side, here // (2 * side)
    same_core = [[2 * i + c for i in range(chips)] for c in range(2)]
    swap = [(i, i ^ 1) for i in range(devices)]

    def to(v, dx, dy):
        return lax.ppermute(
            v,
            "tp",
            [
                ((y * side + x) * 2 + c, ((y + dy) % side * side + (x + dx) % side) * 2 + c)
                for y in range(side)
                for x in range(side)
                for c in range(2)
            ],
        )

    ids = [expert_ids[:, k] for k in range(chosen)]
    hot = [
        (i[:, None] == jnp.arange(groups, dtype=jnp.int32)[None, :]).astype(F32) for i in ids
    ]
    both = sum(hot)
    t = jnp.arange(tok_rows, dtype=jnp.int32)
    before = jnp.dot((t[:, None] > t[None, :]).astype(F32), both)
    place = []
    for k in range(chosen):
        rank = jnp.sum(before * hot[k], axis=1).astype(jnp.int32)
        slot = ids[k] * cap + rank
        place.append((slot[None, :] == jnp.arange(rows, dtype=jnp.int32)[:, None]).astype(BF))
    cot = cotangent.astype(F32)
    weight = [combine_weights[:, k][:, None] for k in range(chosen)]
    send_rows = dot(sum(place), tokens, 1, 0)
    send_grad = sum(dot(place[k], (weight[k] * cot).astype(BF), 1, 0) for k in range(chosen))
    send = jnp.concatenate(
        [send_rows.reshape(groups, cap, width), send_grad.reshape(groups, cap, width)], axis=1
    ).astype(BF)
    recv = lax.all_to_all(send, "ep", 0, 0, tiled=True)
    piece = (
        jnp.concatenate(
            [recv[:, :cap].reshape(rows, width), recv[:, cap:].reshape(rows, width)], axis=0
        )
    ).T

    mine = lax.all_to_all(
        jnp.broadcast_to(piece[None], (chips, *piece.shape)),
        "tp", 0, 0, tiled=True, axis_index_groups=same_core,
    )
    theirs = lax.ppermute(mine, "tp", swap)
    full = jnp.where(
        (jnp.arange(2) == core)[None, :, None, None], mine[:, None], theirs[:, None]
    ).reshape(feats, 2 * rows)
    x, dy = full[:, :rows], full[:, rows:]

    gate_pre = dot(x, wg, 0, 0)
    up_pre = dot(x, wu, 0, 0)
    sigma = jax.nn.sigmoid(gate_pre)
    active = gate_pre * sigma
    slope = sigma * (1.0 + gate_pre * (1.0 - sigma))
    hidden = (active * up_pre).astype(BF)
    grad_hidden = dot(dy, wd, 0, 1)
    ggp = (grad_hidden * up_pre * slope).astype(BF)
    gup = (grad_hidden * active).astype(BF)
    inner = jnp.sum(hidden.astype(F32) * grad_hidden, axis=1)

    half = hid // 2
    factor_a, factor_b = (
        jnp.concatenate([v[:, i * half : (i + 1) * half] for v in (ggp, gup, hidden)], axis=1)
        for i in range(2)
    )
    along_x = [factor_a] + [to(factor_a, d, 0) for d in range(1, side)]
    along_y = [factor_b] + [to(factor_b, 0, d) for d in range(1, side)]
    along_x = [v for f in along_x for v in (f, lax.ppermute(f, "tp", swap))]
    along_y = [v for f in along_y for v in (f, lax.ppermute(f, "tp", swap))]

    keep, give = partials(core[None], hidden, ggp, gup, wg, wu, wd, chips, width)
    got = lax.ppermute(give, "tp", swap)
    inner = inner + lax.ppermute(inner, "tp", swap)
    hi, lo = halves(inner)
    extra = jnp.pad(jnp.stack([hi, lo]), ((0, 6), (0, rows)))
    reduced = add_pair(keep, got, extra)
    summed = jnp.sum(
        lax.all_to_all(
            reduced, "tp", 0, 0, tiled=True, axis_index_groups=same_core
        ).astype(F32),
        axis=0,
    )

    line = jnp.arange(side)
    ys, xs = (cy + line) % side, (cx + line) % side
    grads_a = weight_grads(ys * side + cx, mine, along_x)
    grads_b = weight_grads(cy * side + xs, mine, along_y)
    pieces = [grads_a[0]] + [to(grads_a[d], 0, d) for d in range(1, side)]
    pieces += [grads_b[0]] + [to(grads_b[d], d, 0) for d in range(1, side)]
    ys, xs = (cy - line) % side, (cx - line) % side
    cores = jnp.stack([core, 1 - core])
    from_a = ((ys[:, None] * side + xs[None, :])[:, :, None] * 2 + cores) * hid
    from_b = ((ys[None, :] * side + xs[:, None])[:, :, None] * 2 + cores) * hid + half
    columns = jnp.concatenate([from_a.reshape(-1), from_b.reshape(-1)])

    hi, lo = halves(summed[width] + summed[width + 1])
    back = jnp.concatenate(
        [summed[:width].astype(BF), hi[None], lo[None], jnp.zeros((6, 2 * rows), BF)], axis=0
    ).T.reshape(2, groups, cap, width + 8)
    back = jnp.concatenate([back[0], back[1]], axis=1)
    back = lax.all_to_all(back, "ep", 0, 0, tiled=True)
    out_back = back[:, :cap].reshape(rows, width + 8)
    in_back = back[:, cap:].reshape(rows, width + 8)
    chosen_out = [dot(place[k], out_back, 0, 0) for k in range(chosen)]
    mixed = sum(weight[k] * chosen_out[k][:, :width] for k in range(chosen)).astype(BF)
    grad_combine = jnp.concatenate(
        [
            (chosen_out[k][:, width : width + 1] + chosen_out[k][:, width + 1 : width + 2])
            / weight[k]
            for k in range(chosen)
        ],
        axis=1,
    )
    grad_tokens = dot(sum(place), in_back[:, :width], 0, 0).astype(BF)

    gate_out, up_out, down_out = lay_out(columns, pieces, hid)
    return (
        mixed,
        grad_tokens,
        grad_combine,
        gate_out[None],
        up_out[None],
        down_out.T[None],
    )


def solution(mesh):
    return jax.shard_map(
        body,
        mesh=mesh,
        in_specs=(
            P("ep", "tp"),
            P("ep", "tp"),
            P("ep", None),
            P("ep", None),
            P("ep", None, "tp"),
            P("ep", None, "tp"),
            P("ep", "tp", None),
        ),
        out_specs=(
            P("ep", "tp"),
            P("ep", "tp"),
            P("ep", None),
            P("ep", "tp", None),
            P("ep", "tp", None),
            P("ep", None, "tp"),
        ),
        check_vma=False,
    )
```

```python
import math

import jax
import jax.numpy as jnp
from jax import lax
from jax.experimental import pallas as pl
from jax.experimental.pallas import tpu as pltpu
from jax.sharding import PartitionSpec as P


BF = jnp.bfloat16
F32 = jnp.float32
LIMIT = pltpu.CompilerParams(vmem_limit_bytes=24 * 2**20)


def dot(a, b, ca, cb):
    return lax.dot_general(a, b, (((ca,), (cb,)), ((), ())), preferred_element_type=F32)


def halves(v):
    hi = v.astype(BF)
    return hi, (v - hi.astype(F32)).astype(BF)


def vmem():
    return pl.BlockSpec(memory_space=pltpu.VMEM)


def smem():
    return pl.BlockSpec(memory_space=pltpu.SMEM)


def partials(core, hidden, ggp, gup, wg, wu, wd, chips, width, steps=4):
    rows, hid = hidden.shape
    feats = wg.shape[0]
    block = feats // steps
    each = chips // steps
    lanes = 2 * rows
    pad = 64

    def kernel(core_ref, h_ref, g_ref, u_ref, wg_ref, wu_ref, wd_ref, keep_ref, give_ref, both):
        zeros = jnp.zeros((pad, hid), BF)
        h = jnp.concatenate([h_ref[...], zeros], axis=0)
        g = jnp.concatenate([zeros, g_ref[...]], axis=0)
        u = jnp.concatenate([zeros, u_ref[...]], axis=0)
        out_t = dot(wd_ref[...].T, h, 1, 1)
        in_t = dot(wg_ref[...], g, 1, 1) + dot(wu_ref[...], u, 1, 1)
        mid = rows - pad
        joined = jnp.concatenate(
            [
                out_t[:, :mid],
                out_t[:, mid : mid + 128] + in_t[:, :128],
                in_t[:, 128:],
            ],
            axis=1,
        ).astype(BF)
        both[...] = joined.reshape(each, 2, width, lanes)
        c = core_ref[0]
        for i in range(each):
            keep_ref[i] = both[i, c]
            give_ref[i] = both[i, 1 - c]

    whole = pl.BlockSpec((rows, hid), lambda i: (0, 0))
    out = pl.BlockSpec((each, width, lanes), lambda i: (i, 0, 0))
    return pl.pallas_call(
        kernel,
        grid=(steps,),
        out_shape=[jax.ShapeDtypeStruct((chips, width, lanes), BF)] * 2,
        in_specs=[
            smem(),
            whole,
            whole,
            whole,
            pl.BlockSpec((block, hid), lambda i: (i, 0)),
            pl.BlockSpec((block, hid), lambda i: (i, 0)),
            pl.BlockSpec((hid, block), lambda i: (0, i)),
        ],
        out_specs=[out, out],
        scratch_shapes=[pltpu.VMEM((each, 2, width, lanes), BF)],
        compiler_params=LIMIT,
        name="partials",
    )(core, hidden, ggp, gup, wg, wu, wd)


def add_pair(keep, got, extra, steps=2):
    chips, width, lanes = keep.shape
    more = extra.shape[0]
    each = chips // steps

    def kernel(a, b, e, o):
        o[:, :width] = (a[...].astype(F32) + b[...].astype(F32)).astype(BF)
        for i in range(each):
            o[i, width:] = e[...]

    spec = pl.BlockSpec((each, width, lanes), lambda i: (i, 0, 0))
    return pl.pallas_call(
        kernel,
        grid=(steps,),
        out_shape=jax.ShapeDtypeStruct((chips, width + more, lanes), BF),
        in_specs=[spec, spec, pl.BlockSpec((more, lanes), lambda i: (0, 0))],
        out_specs=pl.BlockSpec((each, width + more, lanes), lambda i: (i, 0, 0)),
        compiler_params=LIMIT,
        name="add_pair",
    )(keep, got, extra)


def extra_rows(v, more):
    hi = v.astype(BF).astype(F32)
    return jnp.concatenate([hi, v - hi, jnp.zeros((more - 2, v.shape[1]), F32)], axis=0)


def finish_sum(parts, width, groups):
    chips, _, lanes = parts.shape
    rows = lanes // 2
    cap = rows // groups

    def kernel(ref, out, turned):
        total = ref[0].astype(F32)
        for i in range(1, chips):
            total += ref[i].astype(F32)
        e = total[width : width + 1] + total[width + 1 : width + 2]
        turned[...] = jnp.concatenate([total[:width], extra_rows(e, 128 - width)], axis=0).T
        for g in range(groups):
            at = g * cap
            out[g] = jnp.concatenate(
                [turned[at : at + cap], turned[rows + at : rows + at + cap]], axis=0
            ).astype(BF)

    return pl.pallas_call(
        kernel,
        out_shape=jax.ShapeDtypeStruct((groups, 2 * cap, 128), BF),
        in_specs=[vmem()],
        out_specs=vmem(),
        scratch_shapes=[pltpu.VMEM((lanes, 128), F32)],
        compiler_params=LIMIT,
        name="finish_sum",
    )(parts)


def assemble(place, mine, theirs):
    side = len(mine)
    wide, lanes = mine[0].shape
    width = wide // side
    chips = side * side

    def kernel(at, *refs):
        full, line = refs[2 * side :]
        x, y, c = at[0], at[1], at[2]

        def chip_of(core, dx, dy):
            across = lax.rem(x + dx + side, side), lax.rem(y + dy + side, side)
            down = lax.rem(x + dy + side, side), lax.rem(y + dx + side, side)
            first = core == 0
            cx = jnp.where(first, across[0], down[0])
            cy = jnp.where(first, across[1], down[1])
            return cy * side + cx

        for q in range(2):
            core = c if q == 0 else 1 - c
            for j in range(side):
                for i in range(side):
                    full[chip_of(core, -i, -j) * 2 + core] = refs[q * side + j][
                        i * width : (i + 1) * width
                    ]
        for q in range(2):
            core = c if q == 0 else 1 - c
            for d in range(side):
                rows = slice((q * side + d) * width, (q * side + d + 1) * width)
                line[rows] = full[chip_of(c, 0, d) * 2 + core]

    return pl.pallas_call(
        kernel,
        out_shape=[
            jax.ShapeDtypeStruct((2 * chips, width, lanes), BF),
            jax.ShapeDtypeStruct((2 * side * width, lanes), BF),
        ],
        in_specs=[smem()] + [vmem()] * (2 * side),
        out_specs=[vmem()] * 2,
        compiler_params=LIMIT,
        name="assemble",
    )(place, *mine, *theirs)


def weight_grads(line, factors, width):
    features, lanes = line.shape
    rows = lanes // 2
    n = len(factors)
    hid = factors[0].shape[1] // 3
    devices = features // width
    pad = 64
    deep = rows + pad

    def kernel(*refs):
        lhs = refs[0]
        fs, outs = refs[1 : 1 + n], refs[1 + n : 1 + n + devices]
        g, h = refs[1 + n + devices :]
        g[rows:] = jnp.zeros((pad, 2 * hid), BF)
        h[:pad] = jnp.zeros((pad, hid), BF)
        for s in range(n):
            g[:rows] = fs[s][:, : 2 * hid]
            h[pad:] = fs[s][:, 2 * hid :]
            rg = dot(lhs[:, :deep], g[...], 1, 0).astype(BF)
            rh = dot(lhs[:, lanes - deep :], h[...], 1, 0).astype(BF)
            for j in range(devices):
                at = slice(j * width, (j + 1) * width)
                o = s * 3 * hid
                outs[j][:, o : o + 2 * hid] = rg[at]
                outs[j][:, o + 2 * hid : o + 3 * hid] = rh[at]

    return pl.pallas_call(
        kernel,
        out_shape=[jax.ShapeDtypeStruct((width, n * 3 * hid), BF)] * devices,
        in_specs=[vmem()] * (1 + n),
        out_specs=[vmem()] * devices,
        scratch_shapes=[pltpu.VMEM((deep, 2 * hid), BF), pltpu.VMEM((deep, hid), BF)],
        compiler_params=LIMIT,
        name="weight_grads",
    )(line, *factors)


def lay_out(columns, pieces, hid, steps=3):
    width, wide = pieces[0].shape
    n = len(pieces)
    per = wide // (3 * hid)
    total = n * per * hid
    block = width // steps

    def kernel(cols, *refs):
        ins, outs = refs[:n], refs[n:]
        for p in range(n):
            for s in range(per):
                at = pl.multiple_of(cols[p * per + s], hid)
                for m in range(3):
                    o = (s * 3 + m) * hid
                    outs[m][:, pl.ds(at, hid)] = ins[p][:, o : o + hid]

    return pl.pallas_call(
        kernel,
        grid=(steps,),
        out_shape=[jax.ShapeDtypeStruct((width, total), BF)] * 3,
        in_specs=[smem()] + [pl.BlockSpec((block, wide), lambda i: (i, 0))] * n,
        out_specs=[pl.BlockSpec((block, total), lambda i: (i, 0))] * 3,
        compiler_params=LIMIT,
        name="lay_out",
    )(columns, *pieces)


def body(tokens, cotangent, expert_ids, combine_weights, w_gate, w_up, w_down):
    groups = lax.axis_size("ep")
    devices = lax.axis_size("tp")
    chips = devices // 2
    tok_rows, width = tokens.shape
    chosen = expert_ids.shape[1]
    cap = tok_rows * chosen * 5 // (3 * groups)
    rows = groups * cap
    wg, wu, wd = w_gate[0], w_up[0], w_down[0]
    hid = wg.shape[1]
    feats = wg.shape[0]
    side = math.isqrt(chips)
    here = lax.axis_index("tp")
    core, cx, cy = here % 2, here // 2 % side, here // (2 * side)
    swap = [(i, i ^ 1) for i in range(devices)]

    def along(v, d, turn=0, other=0):
        pairs = []
        for y in range(side):
            for x in range(side):
                for c in range(2):
                    dx, dy = (d, 0) if c == turn else (0, d)
                    to = ((y + dy) % side * side + (x + dx) % side) * 2 + (c ^ other)
                    pairs.append(((y * side + x) * 2 + c, to))
        return lax.ppermute(v, "tp", pairs)

    def swapped(v):
        return lax.ppermute(v, "tp", swap)

    ids = [expert_ids[:, k] for k in range(chosen)]
    hot = [
        (i[:, None] == jnp.arange(groups, dtype=jnp.int32)[None, :]).astype(F32) for i in ids
    ]
    both = sum(hot)
    t = jnp.arange(tok_rows, dtype=jnp.int32)
    before = jnp.dot((t[:, None] > t[None, :]).astype(F32), both)
    place = []
    for k in range(chosen):
        rank = jnp.sum(before * hot[k], axis=1).astype(jnp.int32)
        slot = ids[k] * cap + rank
        place.append((slot[None, :] == jnp.arange(rows, dtype=jnp.int32)[:, None]).astype(BF))
    cot = cotangent.astype(F32)
    weight = [combine_weights[:, k][:, None] for k in range(chosen)]
    send_rows = dot(sum(place), tokens, 1, 0)
    send_grad = sum(dot(place[k], (weight[k] * cot).astype(BF), 1, 0) for k in range(chosen))
    send = jnp.concatenate(
        [send_rows.reshape(groups, cap, width), send_grad.reshape(groups, cap, width)], axis=1
    ).astype(BF)
    recv = lax.all_to_all(send, "ep", 0, 0, tiled=True)
    piece = (
        jnp.concatenate(
            [recv[:, :cap].reshape(rows, width), recv[:, cap:].reshape(rows, width)], axis=0
        )
    ).T

    place_now = jnp.stack([cx, cy, core])
    steps = (1, 3, 2) if side == 4 else range(1, side)
    order = (0, *steps)

    def line_of(v, turn):
        got = {0: v, **{d: along(v, d, turn) for d in steps}}
        return [got[d] for d in range(side)]

    mine = line_of(jnp.concatenate(line_of(piece, 0)), 1)
    theirs = {d: swapped(mine[d]) for d in order}
    full, line = assemble(place_now, mine, [theirs[d] for d in range(side)])
    full = full.reshape(feats, 2 * rows)
    x, dy = full[:, :rows], full[:, rows:]

    gate_pre = dot(x, wg, 0, 0)
    up_pre = dot(x, wu, 0, 0)
    sigma = jax.nn.sigmoid(gate_pre)
    active = gate_pre * sigma
    slope = sigma * (1.0 + gate_pre * (1.0 - sigma))
    hidden = (active * up_pre).astype(BF)
    grad_hidden = dot(dy, wd, 0, 1)
    ggp = (grad_hidden * up_pre * slope).astype(BF)
    gup = (grad_hidden * active).astype(BF)
    inner = jnp.sum(hidden.astype(F32) * grad_hidden, axis=1)

    factors = line_of(jnp.concatenate([ggp, gup, hidden], axis=1), 0)

    keep, give = partials(core[None], hidden, ggp, gup, wg, wu, wd, chips, width)
    got = swapped(give)
    inner = inner + swapped(inner)
    hi, lo = halves(inner)
    more = 8
    extra = jnp.pad(jnp.stack([hi, lo]), ((0, more - 2), (0, rows)))
    reduced = add_pair(keep, got, extra)
    same_core = [[2 * i + c for i in range(chips)] for c in range(2)]
    parts = lax.all_to_all(
        reduced, "tp", 0, 0, tiled=True, axis_index_groups=same_core
    )
    back = finish_sum(parts, width, groups)

    grads = weight_grads(line, factors, width)
    pieces = {(0, 0): grads[0]}
    for d in (*steps, 0):
        for q in range(2):
            if (q, d) != (0, 0):
                pieces[q, d] = along(grads[q * side + d], d, 1, q)
    r = jnp.arange(side)
    columns = []
    for q in range(2):
        sender = core ^ q
        for d in range(side):
            fx, fy = (cx - r) % side, (cy - d) % side
            tx, ty = (cx - d) % side, (cy - r) % side
            chip = jnp.where(sender == 0, fy * side + fx, ty * side + tx)
            columns.append((chip * 2 + sender) * hid)
    columns = jnp.concatenate(columns)
    pieces = [pieces[q, d] for q in range(2) for d in range(side)]

    back = lax.all_to_all(back, "ep", 0, 0, tiled=True)
    out_back = back[:, :cap].reshape(rows, -1)
    in_back = back[:, cap:].reshape(rows, -1)
    chosen_out = [dot(place[k], out_back, 0, 0) for k in range(chosen)]
    mixed = sum(weight[k] * chosen_out[k][:, :width] for k in range(chosen)).astype(BF)
    grad_combine = jnp.concatenate(
        [
            (chosen_out[k][:, width : width + 1] + chosen_out[k][:, width + 1 : width + 2])
            / weight[k]
            for k in range(chosen)
        ],
        axis=1,
    )
    grad_tokens = dot(sum(place), in_back[:, :width], 0, 0).astype(BF)

    gate_out, up_out, down_out = lay_out(columns, pieces, hid)
    return (
        mixed,
        grad_tokens,
        grad_combine,
        gate_out[None],
        up_out[None],
        down_out.T[None],
    )


def solution(mesh):
    return jax.shard_map(
        body,
        mesh=mesh,
        in_specs=(
            P("ep", "tp"),
            P("ep", "tp"),
            P("ep", None),
            P("ep", None),
            P("ep", None, "tp"),
            P("ep", None, "tp"),
            P("ep", "tp", None),
        ),
        out_specs=(
            P("ep", "tp"),
            P("ep", "tp"),
            P("ep", None),
            P("ep", "tp", None),
            P("ep", "tp", None),
            P("ep", None, "tp"),
        ),
        check_vma=False,
    )
```

```python
import math

import jax
import jax.numpy as jnp
from jax import lax
from jax.experimental import pallas as pl
from jax.experimental.pallas import tpu as pltpu
from jax.sharding import PartitionSpec as P


BF = jnp.bfloat16
F32 = jnp.float32
LIMIT = pltpu.CompilerParams(vmem_limit_bytes=24 * 2**20)


def dot(a, b, ca, cb):
    return lax.dot_general(a, b, (((ca,), (cb,)), ((), ())), preferred_element_type=F32)


def halves(v):
    hi = v.astype(BF)
    return hi, (v - hi.astype(F32)).astype(BF)


def vmem():
    return pl.BlockSpec(memory_space=pltpu.VMEM)


def smem():
    return pl.BlockSpec(memory_space=pltpu.SMEM)


def placed(ids_ref, groups, cap):
    chosen, n = ids_ref.shape
    ids = [ids_ref[k : k + 1] for k in range(chosen)]
    expert = lax.broadcasted_iota(jnp.int32, (groups, n), 0)
    hot = [(i == expert).astype(F32) for i in ids]
    t, u = (lax.broadcasted_iota(jnp.int32, (n, n), d) for d in range(2))
    before = dot(sum(hot).astype(BF), (t < u).astype(BF), 1, 0)
    slots = [
        i * cap + jnp.sum(before * h, axis=0, keepdims=True).astype(jnp.int32)
        for i, h in zip(ids, hot)
    ]
    return slots, t == u


def column(eye, row):
    return jnp.sum(jnp.where(eye, row, jnp.zeros_like(row)), axis=1, keepdims=True)


def dispatch(tokens, cotangent, ids, weights, groups, cap):
    n, width = tokens.shape
    chosen = ids.shape[0]
    rows = groups * cap

    def kernel(tok, cot, ids_ref, w_ref, out):
        slots, eye = placed(ids_ref, groups, cap)
        at = lax.broadcasted_iota(jnp.int32, (rows, n), 0)
        place = [(at == s).astype(F32).astype(BF) for s in slots]
        grads = cot[...].astype(F32)
        sent = dot(sum(place), tok[...], 1, 0)
        grad = sum(
            dot(place[k], (column(eye, w_ref[k : k + 1]) * grads).astype(BF), 1, 0)
            for k in range(chosen)
        )
        for g in range(groups):
            part = slice(g * cap, (g + 1) * cap)
            out[g] = jnp.concatenate([sent[part], grad[part]], axis=0).astype(BF)

    return pl.pallas_call(
        kernel,
        out_shape=jax.ShapeDtypeStruct((groups, 2 * cap, width), BF),
        in_specs=[vmem()] * 4,
        out_specs=vmem(),
        name="dispatch",
    )(tokens, cotangent, ids, weights)


def mix(back, ids, weights, width):
    groups, both, lanes = back.shape
    cap = both // 2
    rows = groups * cap
    chosen, n = ids.shape

    def kernel(ref, ids_ref, w_ref, mixed, grad, combine):
        slots, eye = placed(ids_ref, groups, cap)
        at = lax.broadcasted_iota(jnp.int32, (n, rows), 1)
        place = [(at == column(eye, s)).astype(F32).astype(BF) for s in slots]
        blocks = [ref[g].astype(F32) for g in range(groups)]
        outs = jnp.concatenate([b[:cap] for b in blocks], axis=0).astype(BF)
        ins = jnp.concatenate([b[cap:] for b in blocks], axis=0).astype(BF)
        total = jnp.zeros((n, lanes), F32)
        for k in range(chosen):
            weight = w_ref[k : k + 1]
            out = dot(place[k], outs, 1, 0)
            total += column(eye, weight) * out
            inner = out[:, width : width + 1] + out[:, width + 1 : width + 2]
            inner = jnp.sum(jnp.where(eye, inner, 0.0), axis=0, keepdims=True)
            combine[k : k + 1] = inner / weight
        mixed[...] = total[:, :width].astype(BF)
        grad[...] = dot(sum(place), ins, 1, 0)[:, :width].astype(BF)

    return pl.pallas_call(
        kernel,
        out_shape=[jax.ShapeDtypeStruct((n, width), BF)] * 2
        + [jax.ShapeDtypeStruct((chosen, n), F32)],
        in_specs=[vmem()] * 3,
        out_specs=[vmem()] * 3,
        compiler_params=LIMIT,
        name="mix",
    )(back, ids, weights)


def partials(core, hidden, ggp, gup, wg, wu, wd, chips, width, steps=4):
    rows, hid = hidden.shape
    feats = wg.shape[0]
    block = feats // steps
    each = chips // steps
    lanes = 2 * rows
    pad = 64

    def kernel(core_ref, h_ref, g_ref, u_ref, wg_ref, wu_ref, wd_ref, keep_ref, give_ref, both):
        zeros = jnp.zeros((pad, hid), BF)
        h = jnp.concatenate([h_ref[...], zeros], axis=0)
        g = jnp.concatenate([zeros, g_ref[...]], axis=0)
        u = jnp.concatenate([zeros, u_ref[...]], axis=0)
        out_t = dot(wd_ref[...].T, h, 1, 1)
        in_t = dot(wg_ref[...], g, 1, 1) + dot(wu_ref[...], u, 1, 1)
        mid = rows - pad
        joined = jnp.concatenate(
            [
                out_t[:, :mid],
                out_t[:, mid : mid + 128] + in_t[:, :128],
                in_t[:, 128:],
            ],
            axis=1,
        ).astype(BF)
        both[...] = joined.reshape(each, 2, width, lanes)
        c = core_ref[0]
        for i in range(each):
            keep_ref[i] = both[i, c]
            give_ref[i] = both[i, 1 - c]

    whole = pl.BlockSpec((rows, hid), lambda i: (0, 0))
    out = pl.BlockSpec((each, width, lanes), lambda i: (i, 0, 0))
    return pl.pallas_call(
        kernel,
        grid=(steps,),
        out_shape=[jax.ShapeDtypeStruct((chips, width, lanes), BF)] * 2,
        in_specs=[
            smem(),
            whole,
            whole,
            whole,
            pl.BlockSpec((block, hid), lambda i: (i, 0)),
            pl.BlockSpec((block, hid), lambda i: (i, 0)),
            pl.BlockSpec((hid, block), lambda i: (0, i)),
        ],
        out_specs=[out, out],
        scratch_shapes=[pltpu.VMEM((each, 2, width, lanes), BF)],
        compiler_params=LIMIT,
        name="partials",
    )(core, hidden, ggp, gup, wg, wu, wd)


def add_pair(place, keep, got, extra):
    chips, width, lanes = keep.shape
    more = extra.shape[0]
    side = math.isqrt(chips)

    def kernel(at, a, b, e, *outs):
        first = at[2] == 0
        for j in range(side):
            y, x = lax.rem(at[1] + j, side), lax.rem(at[0] + j, side)
            for i in range(side):
                chip = jnp.where(first, y * side + i, i * side + x)
                total = (a[chip].astype(F32) + b[chip].astype(F32)).astype(BF)
                outs[j][i * width : (i + 1) * width] = total
            outs[j][side * width :] = e[...]

    return pl.pallas_call(
        kernel,
        out_shape=[jax.ShapeDtypeStruct((side * width + more, lanes), BF)] * side,
        in_specs=[smem(), vmem(), vmem(), vmem()],
        out_specs=[vmem()] * side,
        compiler_params=LIMIT,
        name="add_pair",
    )(place, keep, got, extra)


def add_line(place, blocks, width):
    side = len(blocks)
    deep, lanes = blocks[0].shape
    more = deep - side * width

    def kernel(at, *refs):
        ins, outs = refs[:side], refs[side:]
        mine = jnp.where(at[2] == 0, at[0], at[1])
        e = sum(r[side * width :].astype(F32) for r in ins)
        e = extra_rows(e[0:1] + e[1:2], more).astype(BF)
        for j in range(side):
            rows = pl.ds(pl.multiple_of(lax.rem(mine + j, side) * width, 16), width)
            total = ins[0][rows].astype(F32)
            for r in ins[1:]:
                total += r[rows].astype(F32)
            outs[j][:width] = total.astype(BF)
            outs[j][width:] = e

    return pl.pallas_call(
        kernel,
        out_shape=[jax.ShapeDtypeStruct((width + more, lanes), BF)] * side,
        in_specs=[smem()] + [vmem()] * side,
        out_specs=[vmem()] * side,
        compiler_params=LIMIT,
        name="add_line",
    )(place, *blocks)


def extra_rows(v, more):
    hi = v.astype(BF).astype(F32)
    return jnp.concatenate([hi, v - hi, jnp.zeros((more - 2, v.shape[1]), F32)], axis=0)


def finish_sum(parts, width, groups):
    n = len(parts)
    lanes = parts[0].shape[1]
    rows = lanes // 2
    cap = rows // groups

    def kernel(*refs):
        out, turned = refs[n:]
        total = sum(r[...].astype(F32) for r in refs[:n])
        e = total[width : width + 1] + total[width + 1 : width + 2]
        turned[...] = jnp.concatenate([total[:width], extra_rows(e, 128 - width)], axis=0).T
        for g in range(groups):
            at = g * cap
            out[g] = jnp.concatenate(
                [turned[at : at + cap], turned[rows + at : rows + at + cap]], axis=0
            ).astype(BF)

    return pl.pallas_call(
        kernel,
        out_shape=jax.ShapeDtypeStruct((groups, 2 * cap, 128), BF),
        in_specs=[vmem()] * n,
        out_specs=vmem(),
        scratch_shapes=[pltpu.VMEM((lanes, 128), F32)],
        compiler_params=LIMIT,
        name="finish_sum",
    )(*parts)


def assemble(place, mine, theirs):
    side = len(mine)
    wide, lanes = mine[0].shape
    width = wide // side
    chips = side * side
    n = 2 * side

    def kernel(at, *refs):
        full, line, held, sems = refs[n:]
        x, y, c = at[0], at[1], at[2]
        copies = [pltpu.make_async_copy(refs[p], held.at[p], sems.at[p]) for p in range(n)]
        for one in copies:
            one.start()
        for q in range(2):
            core = c if q == 0 else 1 - c
            first = core == 0
            for j in range(side):
                copies[q * side + j].wait()
                for i in range(side):
                    x_of = jnp.where(first, x - i, x - j)
                    y_of = jnp.where(first, y - j, y - i)
                    chip = lax.rem(y_of + side, side) * side + lax.rem(x_of + side, side)
                    full[chip * 2 + core] = held[q * side + j, i * width : (i + 1) * width]
        for d in range(side):
            back = (side - d) % side
            line[d * width : (d + 1) * width] = held[back, :width]
            line[(side + d) * width : (side + d + 1) * width] = held[
                side, back * width : (back + 1) * width
            ]

    return pl.pallas_call(
        kernel,
        out_shape=[
            jax.ShapeDtypeStruct((2 * chips, width, lanes), BF),
            jax.ShapeDtypeStruct((n * width, lanes), BF),
        ],
        in_specs=[smem()] + [pl.BlockSpec(memory_space=pltpu.HBM)] * n,
        out_specs=[vmem()] * 2,
        scratch_shapes=[
            pltpu.VMEM((n, wide, lanes), BF),
            pltpu.SemaphoreType.DMA((n,)),
        ],
        compiler_params=LIMIT,
        name="assemble",
    )(place, *mine, *theirs)


def weight_grads(line, factors, width):
    features, lanes = line.shape
    rows = lanes // 2
    n = len(factors)
    hid = factors[0].shape[1] // 3
    devices = features // width
    pad = 64
    deep = rows + pad

    def kernel(*refs):
        lhs = refs[0]
        fs, outs = refs[1 : 1 + n], refs[1 + n : 1 + n + devices]
        g, h = refs[1 + n + devices :]
        g[rows:] = jnp.zeros((pad, 2 * hid), BF)
        h[:pad] = jnp.zeros((pad, hid), BF)
        for s in range(n):
            g[:rows] = fs[s][:, : 2 * hid]
            h[pad:] = fs[s][:, 2 * hid :]
            rg = dot(lhs[:, :deep], g[...], 1, 0).astype(BF)
            rh = dot(lhs[:, lanes - deep :], h[...], 1, 0).astype(BF)
            for j in range(devices):
                at = slice(j * width, (j + 1) * width)
                o = s * 3 * hid
                outs[j][:, o : o + 2 * hid] = rg[at]
                outs[j][:, o + 2 * hid : o + 3 * hid] = rh[at]

    return pl.pallas_call(
        kernel,
        out_shape=[jax.ShapeDtypeStruct((width, n * 3 * hid), BF)] * devices,
        in_specs=[vmem()] * (1 + n),
        out_specs=[vmem()] * devices,
        scratch_shapes=[pltpu.VMEM((deep, 2 * hid), BF), pltpu.VMEM((deep, hid), BF)],
        compiler_params=LIMIT,
        name="weight_grads",
    )(line, *factors)


def lay_out(columns, pieces, hid, steps=3):
    width, wide = pieces[0].shape
    n = len(pieces)
    per = wide // (3 * hid)
    total = n * per * hid
    block = width // steps

    def kernel(cols, *refs):
        ins, outs = refs[:n], refs[n:]
        for p in range(n):
            for s in range(per):
                at = pl.multiple_of(cols[p * per + s], hid)
                for m in range(3):
                    o = (s * 3 + m) * hid
                    outs[m][:, pl.ds(at, hid)] = ins[p][:, o : o + hid]

    return pl.pallas_call(
        kernel,
        grid=(steps,),
        out_shape=[jax.ShapeDtypeStruct((width, total), BF)] * 3,
        in_specs=[smem()] + [pl.BlockSpec((block, wide), lambda i: (i, 0))] * n,
        out_specs=[pl.BlockSpec((block, total), lambda i: (i, 0))] * 3,
        compiler_params=LIMIT,
        name="lay_out",
    )(columns, *pieces)


def body(tokens, cotangent, expert_ids, combine_weights, w_gate, w_up, w_down):
    groups = lax.axis_size("ep")
    devices = lax.axis_size("tp")
    chips = devices // 2
    tok_rows, width = tokens.shape
    chosen = expert_ids.shape[1]
    cap = tok_rows * chosen * 5 // (3 * groups)
    rows = groups * cap
    wg, wu, wd = w_gate[0], w_up[0], w_down[0]
    hid = wg.shape[1]
    feats = wg.shape[0]
    side = math.isqrt(chips)
    here = lax.axis_index("tp")
    core, cx, cy = here % 2, here // 2 % side, here // (2 * side)
    swap = [(i, i ^ 1) for i in range(devices)]

    def along(v, d, turn=0, other=0):
        pairs = []
        for y in range(side):
            for x in range(side):
                for c in range(2):
                    dx, dy = (d, 0) if c == turn else (0, d)
                    to = ((y + dy) % side * side + (x + dx) % side) * 2 + (c ^ other)
                    pairs.append(((y * side + x) * 2 + c, to))
        return lax.ppermute(v, "tp", pairs)

    def swapped(v):
        return lax.ppermute(v, "tp", swap)

    ids, weights = expert_ids.T, combine_weights.T
    send = dispatch(tokens, cotangent, ids, weights, groups, cap)
    recv = lax.all_to_all(send, "ep", 0, 0, tiled=True)
    piece = (
        jnp.concatenate(
            [recv[:, :cap].reshape(rows, width), recv[:, cap:].reshape(rows, width)], axis=0
        )
    ).T

    place_now = jnp.stack([cx, cy, core])
    steps = (1, 3, 2) if side == 4 else range(1, side)
    order = (0, *steps)

    def line_of(v, turn):
        got = {0: v, **{d: along(v, d, turn) for d in steps}}
        return [got[d] for d in range(side)]

    mine = line_of(jnp.concatenate(line_of(piece, 0)), 1)
    theirs = {d: swapped(mine[d]) for d in order}
    full, line = assemble(place_now, mine, [theirs[d] for d in range(side)])
    full = full.reshape(feats, 2 * rows)
    x, dy = full[:, :rows], full[:, rows:]

    gate_pre = dot(x, wg, 0, 0)
    up_pre = dot(x, wu, 0, 0)
    sigma = jax.nn.sigmoid(gate_pre)
    active = gate_pre * sigma
    slope = sigma * (1.0 + gate_pre * (1.0 - sigma))
    hidden = (active * up_pre).astype(BF)
    grad_hidden = dot(dy, wd, 0, 1)
    ggp = (grad_hidden * up_pre * slope).astype(BF)
    gup = (grad_hidden * active).astype(BF)
    inner = jnp.sum(hidden.astype(F32) * grad_hidden, axis=1)

    factors = line_of(jnp.concatenate([ggp, gup, hidden], axis=1), 0)

    keep, give = partials(core[None], hidden, ggp, gup, wg, wu, wd, chips, width)
    got = swapped(give)
    inner = inner + swapped(inner)
    hi, lo = halves(inner)
    more = 16
    extra = jnp.pad(jnp.stack([hi, lo]), ((0, more - 2), (0, rows)))
    blocks = add_pair(place_now, keep, got, extra)

    def exchanged(blocks, turn):
        return [blocks[0]] + [along(blocks[d], d, turn) for d in range(1, side)]

    blocks = exchanged(blocks, 1)
    blocks = add_line(place_now, blocks, width)
    parts = exchanged(blocks, 0)
    back = finish_sum(parts, width, groups)

    grads = weight_grads(line, factors, width)
    pieces = {(0, 0): grads[0]}
    for d in (*steps, 0):
        for q in range(2):
            if (q, d) != (0, 0):
                pieces[q, d] = along(grads[q * side + d], d, 1, q)
    r = jnp.arange(side)
    columns = []
    for q in range(2):
        sender = core ^ q
        for d in range(side):
            fx, fy = (cx - r) % side, (cy - d) % side
            tx, ty = (cx - d) % side, (cy - r) % side
            chip = jnp.where(sender == 0, fy * side + fx, ty * side + tx)
            columns.append((chip * 2 + sender) * hid)
    columns = jnp.concatenate(columns)
    pieces = [pieces[q, d] for q in range(2) for d in range(side)]

    back = lax.all_to_all(back, "ep", 0, 0, tiled=True)
    mixed, grad_tokens, grad_combine = mix(back, ids, weights, width)

    gate_out, up_out, down_out = lay_out(columns, pieces, hid)
    return (
        mixed,
        grad_tokens,
        grad_combine.T,
        gate_out[None],
        up_out[None],
        down_out.T[None],
    )


def solution(mesh):
    return jax.shard_map(
        body,
        mesh=mesh,
        in_specs=(
            P("ep", "tp"),
            P("ep", "tp"),
            P("ep", None),
            P("ep", None),
            P("ep", None, "tp"),
            P("ep", None, "tp"),
            P("ep", "tp", None),
        ),
        out_specs=(
            P("ep", "tp"),
            P("ep", "tp"),
            P("ep", None),
            P("ep", "tp", None),
            P("ep", "tp", None),
            P("ep", None, "tp"),
        ),
        check_vma=False,
    )
```

```python
import math

import jax
import jax.numpy as jnp
from jax import lax
from jax.experimental import pallas as pl
from jax.experimental.pallas import tpu as pltpu
from jax.sharding import PartitionSpec as P


BF = jnp.bfloat16
F32 = jnp.float32
LIMIT = pltpu.CompilerParams(vmem_limit_bytes=24 * 2**20)


def dot(a, b, ca, cb):
    return lax.dot_general(a, b, (((ca,), (cb,)), ((), ())), preferred_element_type=F32)


def vmem():
    return pl.BlockSpec(memory_space=pltpu.VMEM)


def smem():
    return pl.BlockSpec(memory_space=pltpu.SMEM)


def placed(ids_ref, groups, cap):
    chosen, n = ids_ref.shape
    ids = [ids_ref[k : k + 1] for k in range(chosen)]
    expert = lax.broadcasted_iota(jnp.int32, (groups, n), 0)
    hot = [(i == expert).astype(F32) for i in ids]
    t, u = (lax.broadcasted_iota(jnp.int32, (n, n), d) for d in range(2))
    before = dot(sum(hot).astype(BF), (t < u).astype(BF), 1, 0)
    slots = [
        i * cap + jnp.sum(before * h, axis=0, keepdims=True).astype(jnp.int32)
        for i, h in zip(ids, hot)
    ]
    return slots, t == u


def column(eye, row):
    return jnp.sum(jnp.where(eye, row, jnp.zeros_like(row)), axis=1, keepdims=True)


def dispatch(tokens, cotangent, ids, weights, groups, cap):
    n, width = tokens.shape
    chosen = ids.shape[0]
    rows = groups * cap

    def kernel(tok, cot, ids_ref, w_ref, out):
        slots, eye = placed(ids_ref, groups, cap)
        at = lax.broadcasted_iota(jnp.int32, (rows, n), 0)
        place = [(at == s).astype(F32).astype(BF) for s in slots]
        grads = cot[...].astype(F32)
        sent = dot(sum(place), tok[...], 1, 0)
        grad = sum(
            dot(place[k], (column(eye, w_ref[k : k + 1]) * grads).astype(BF), 1, 0)
            for k in range(chosen)
        )
        for g in range(groups):
            part = slice(g * cap, (g + 1) * cap)
            out[g] = jnp.concatenate([sent[part], grad[part]], axis=0).astype(BF)

    return pl.pallas_call(
        kernel,
        out_shape=jax.ShapeDtypeStruct((groups, 2 * cap, width), BF),
        in_specs=[vmem()] * 4,
        out_specs=vmem(),
        name="dispatch",
    )(tokens, cotangent, ids, weights)


def mix(back, ids, weights, width):
    groups, both, lanes = back.shape
    cap = both // 2
    rows = groups * cap
    chosen, n = ids.shape

    def kernel(ref, ids_ref, w_ref, mixed, grad, combine):
        slots, eye = placed(ids_ref, groups, cap)
        at = lax.broadcasted_iota(jnp.int32, (n, rows), 1)
        place = [(at == column(eye, s)).astype(F32).astype(BF) for s in slots]
        blocks = [ref[g].astype(F32) for g in range(groups)]
        outs = jnp.concatenate([b[:cap] for b in blocks], axis=0).astype(BF)
        ins = jnp.concatenate([b[cap:] for b in blocks], axis=0).astype(BF)
        total = jnp.zeros((n, lanes), F32)
        for k in range(chosen):
            weight = w_ref[k : k + 1]
            out = dot(place[k], outs, 1, 0)
            total += column(eye, weight) * out
            inner = out[:, width : width + 1] + out[:, width + 1 : width + 2]
            inner = jnp.sum(jnp.where(eye, inner, 0.0), axis=0, keepdims=True)
            combine[k : k + 1] = inner / weight
        mixed[...] = total[:, :width].astype(BF)
        grad[...] = dot(sum(place), ins, 1, 0)[:, :width].astype(BF)

    return pl.pallas_call(
        kernel,
        out_shape=[jax.ShapeDtypeStruct((n, width), BF)] * 2
        + [jax.ShapeDtypeStruct((chosen, n), F32)],
        in_specs=[vmem()] * 3,
        out_specs=[vmem()] * 3,
        compiler_params=LIMIT,
        name="mix",
    )(back, ids, weights)


def partials(core, factors, wg, wu, wd_t, chips, width, steps=4):
    rows = factors.shape[0]
    feats, hid = wg.shape
    block = feats // steps
    each = chips // steps
    lanes = 2 * rows
    pad = 64

    def kernel(core_ref, f_ref, wg_ref, wu_ref, wd_ref, keep_ref, give_ref, both):
        zeros = jnp.zeros((pad, hid), BF)
        g = jnp.concatenate([zeros, f_ref[:, :hid]], axis=0)
        u = jnp.concatenate([zeros, f_ref[:, hid : 2 * hid]], axis=0)
        h = jnp.concatenate([f_ref[:, 2 * hid :], zeros], axis=0)
        out_t = dot(wd_ref[...], h, 1, 1)
        in_t = dot(wg_ref[...], g, 1, 1) + dot(wu_ref[...], u, 1, 1)
        mid = rows - pad
        joined = jnp.concatenate(
            [
                out_t[:, :mid],
                out_t[:, mid : mid + 128] + in_t[:, :128],
                in_t[:, 128:],
            ],
            axis=1,
        ).astype(BF)
        both[...] = joined.reshape(each, 2, width, lanes)
        c = core_ref[0]
        for i in range(each):
            keep_ref[i] = both[i, c]
            give_ref[i] = both[i, 1 - c]

    weights = pl.BlockSpec((block, hid), lambda i: (i, 0))
    out = pl.BlockSpec((each, width, lanes), lambda i: (i, 0, 0))
    return pl.pallas_call(
        kernel,
        grid=(steps,),
        out_shape=[jax.ShapeDtypeStruct((chips, width, lanes), BF)] * 2,
        in_specs=[
            smem(),
            pl.BlockSpec((rows, 3 * hid), lambda i: (0, 0)),
            weights,
            weights,
            weights,
        ],
        out_specs=[out, out],
        scratch_shapes=[pltpu.VMEM((each, 2, width, lanes), BF)],
        compiler_params=LIMIT,
        name="partials",
    )(core, factors, wg, wu, wd_t)


def add_pair(place, keep, got, inner, inner_got, more):
    chips, width, lanes = keep.shape
    side = math.isqrt(chips)

    def kernel(at, a, b, inner_a, inner_b, *outs):
        first = at[2] == 0
        extra = extra_rows(inner_a[...] + inner_b[...], more).astype(BF)
        for j in range(side):
            y, x = lax.rem(at[1] + j, side), lax.rem(at[0] + j, side)
            for i in range(side):
                chip = jnp.where(first, y * side + i, i * side + x)
                total = (a[chip].astype(F32) + b[chip].astype(F32)).astype(BF)
                outs[j][i * width : (i + 1) * width] = total
            outs[j][side * width :] = extra

    return pl.pallas_call(
        kernel,
        out_shape=[jax.ShapeDtypeStruct((side * width + more, lanes), BF)] * side,
        in_specs=[smem()] + [vmem()] * 4,
        out_specs=[vmem()] * side,
        compiler_params=LIMIT,
        name="add_pair",
    )(place, keep, got, inner, inner_got)


def add_line(place, blocks, width):
    side = len(blocks)
    deep, lanes = blocks[0].shape
    more = deep - side * width

    def kernel(at, *refs):
        ins, outs = refs[:side], refs[side:]
        mine = jnp.where(at[2] == 0, at[0], at[1])
        e = sum(r[side * width :].astype(F32) for r in ins)
        e = extra_rows(e[0:1] + e[1:2], more).astype(BF)
        for j in range(side):
            rows = pl.ds(pl.multiple_of(lax.rem(mine + j, side) * width, 16), width)
            total = ins[0][rows].astype(F32)
            for r in ins[1:]:
                total += r[rows].astype(F32)
            outs[j][:width] = total.astype(BF)
            outs[j][width:] = e

    return pl.pallas_call(
        kernel,
        out_shape=[jax.ShapeDtypeStruct((width + more, lanes), BF)] * side,
        in_specs=[smem()] + [vmem()] * side,
        out_specs=[vmem()] * side,
        compiler_params=LIMIT,
        name="add_line",
    )(place, *blocks)


def extra_rows(v, more):
    hi = v.astype(BF).astype(F32)
    return jnp.concatenate([hi, v - hi, jnp.zeros((more - 2, v.shape[1]), F32)], axis=0)


def finish_sum(parts, width, groups):
    n = len(parts)
    lanes = parts[0].shape[1]
    rows = lanes // 2
    cap = rows // groups

    def kernel(*refs):
        out, turned = refs[n:]
        total = sum(r[...].astype(F32) for r in refs[:n])
        e = total[width : width + 1] + total[width + 1 : width + 2]
        turned[...] = jnp.concatenate([total[:width], extra_rows(e, 128 - width)], axis=0).T
        for g in range(groups):
            at = g * cap
            out[g] = jnp.concatenate(
                [turned[at : at + cap], turned[rows + at : rows + at + cap]], axis=0
            ).astype(BF)

    return pl.pallas_call(
        kernel,
        out_shape=jax.ShapeDtypeStruct((groups, 2 * cap, 128), BF),
        in_specs=[vmem()] * n,
        out_specs=vmem(),
        scratch_shapes=[pltpu.VMEM((lanes, 128), F32)],
        compiler_params=LIMIT,
        name="finish_sum",
    )(*parts)


def hbm():
    return pl.BlockSpec(memory_space=pltpu.HBM)


def early(place, pieces, later, wg, wu, wd, width):
    feats, hid = wg.shape
    wide, lanes = pieces[0][2].shape
    side = wide // width
    rows = lanes // 2
    n = len(pieces)

    def kernel(at, *refs):
        given = refs[:n]
        g_ref, u_ref, d_ref, ax, ad, ahead, turned, held, weights, sems = refs[n:]
        x, y, c = at[0], at[1], at[2]
        copies = [pltpu.make_async_copy(given[p], held.at[p], sems.at[p]) for p in range(n)]
        for one in copies:
            one.start()
        step = feats // 4
        for i in range(4):
            turned[i * step : (i + 1) * step] = d_ref[:, i * step : (i + 1) * step].T

        def put(q, j, to):
            core = c if q == 0 else 1 - c
            first = core == 0
            for i in range(side):
                x_of = jnp.where(first, x - i, x - j)
                y_of = jnp.where(first, y - j, y - i)
                chip = lax.rem(y_of + side, side) * side + lax.rem(x_of + side, side)
                block = pl.ds(pl.multiple_of((chip * 2 + core) * width, 16), width)
                here = slice(i * width, (i + 1) * width)
                to[here, :hid] = g_ref[block]
                to[here, hid : 2 * hid] = u_ref[block]
                to[here, 2 * hid :] = turned[block]

        for p, (q, j) in enumerate(later):
            put(q, j, ahead.at[p])
        for p in range(n):
            put(pieces[p][0], pieces[p][1], weights)
            copies[p].wait()
            left = held[p].T
            by_x = dot(left[:rows], weights[:, : 2 * hid], 1, 0)
            by_d = dot(left[rows:], weights[:, 2 * hid :], 1, 0)
            ax[...] = by_x if p == 0 else ax[...] + by_x
            ad[...] = by_d if p == 0 else ad[...] + by_d

    return pl.pallas_call(
        kernel,
        out_shape=[
            jax.ShapeDtypeStruct((rows, 2 * hid), F32),
            jax.ShapeDtypeStruct((rows, hid), F32),
            jax.ShapeDtypeStruct((len(later), wide, 3 * hid), BF),
            jax.ShapeDtypeStruct((feats, hid), BF),
        ],
        in_specs=[smem()] + [hbm()] * n + [vmem()] * 3,
        out_specs=[vmem()] * 4,
        scratch_shapes=[
            pltpu.VMEM((n, wide, lanes), BF),
            pltpu.VMEM((wide, 3 * hid), BF),
            pltpu.SemaphoreType.DMA((n,)),
        ],
        compiler_params=LIMIT,
        name="early",
    )(place, *[p[2] for p in pieces], wg, wu, wd)


def late(pieces, ax, ad, weights, mine, theirs, width):
    n = len(pieces)
    side = len(mine)
    wide, lanes = pieces[0].shape
    rows, hid = ad.shape

    def kernel(*refs):
        own, other = refs[n : n + side], refs[n + side]
        ax_ref, ad_ref, w_ref, out, inner, line, held, sems = refs[n + side + 1 :]
        copies = [pltpu.make_async_copy(refs[p], held.at[p], sems.at[p]) for p in range(n)]
        for d in range(side):
            back = (side - d) % side
            for src, to in (
                (own[back].at[pl.ds(0, width)], d),
                (other.at[pl.ds(back * width, width)], side + d),
            ):
                dst = line.at[pl.ds(to * width, width)]
                copies.append(pltpu.make_async_copy(src, dst, sems.at[n + to]))
        for one in copies:
            one.start()
        pre, grad = ax_ref[...], ad_ref[...]
        for p in range(n):
            copies[p].wait()
            left = held[p].T
            pre += dot(left[:rows], w_ref[p, :, : 2 * hid], 1, 0)
            grad += dot(left[rows:], w_ref[p, :, 2 * hid :], 1, 0)
        gate, up = pre[:, :hid], pre[:, hid:]
        sigma = jax.nn.sigmoid(gate)
        active = gate * sigma
        slope = sigma * (1.0 + gate * (1.0 - sigma))
        hidden = (active * up).astype(BF)
        out[:, :hid] = (grad * up * slope).astype(BF)
        out[:, hid : 2 * hid] = (grad * active).astype(BF)
        out[:, 2 * hid :] = hidden
        each = hidden.astype(F32) * grad
        each = jnp.concatenate([each, jnp.zeros((lanes - rows, hid), F32)], axis=0)
        inner[...] = jnp.sum(each.T, axis=0, keepdims=True)
        for one in copies[n:]:
            one.wait()

    return pl.pallas_call(
        kernel,
        out_shape=[
            jax.ShapeDtypeStruct((rows, 3 * hid), BF),
            jax.ShapeDtypeStruct((1, lanes), F32),
            jax.ShapeDtypeStruct((2 * side * width, lanes), BF),
        ],
        in_specs=[hbm()] * (n + side + 1) + [vmem()] * 3,
        out_specs=[vmem()] * 3,
        scratch_shapes=[
            pltpu.VMEM((n, wide, lanes), BF),
            pltpu.SemaphoreType.DMA((n + 2 * side,)),
        ],
        compiler_params=LIMIT,
        name="late",
    )(*pieces, *mine, theirs, ax, ad, weights)


def weight_grads(line, factors, width):
    features, lanes = line.shape
    rows = lanes // 2
    n = len(factors)
    hid = factors[0].shape[1] // 3
    devices = features // width
    pad = 64
    deep = rows + pad

    def kernel(*refs):
        lhs = refs[0]
        fs, outs = refs[1 : 1 + n], refs[1 + n : 1 + n + devices]
        g, h = refs[1 + n + devices :]
        g[rows:] = jnp.zeros((pad, 2 * hid), BF)
        h[:pad] = jnp.zeros((pad, hid), BF)
        for s in range(n):
            g[:rows] = fs[s][:, : 2 * hid]
            h[pad:] = fs[s][:, 2 * hid :]
            rg = dot(lhs[:, :deep], g[...], 1, 0).astype(BF)
            rh = dot(lhs[:, lanes - deep :], h[...], 1, 0).astype(BF)
            for j in range(devices):
                at = slice(j * width, (j + 1) * width)
                o = s * 3 * hid
                outs[j][:, o : o + 2 * hid] = rg[at]
                outs[j][:, o + 2 * hid : o + 3 * hid] = rh[at]

    return pl.pallas_call(
        kernel,
        out_shape=[jax.ShapeDtypeStruct((width, n * 3 * hid), BF)] * devices,
        in_specs=[vmem()] * (1 + n),
        out_specs=[vmem()] * devices,
        scratch_shapes=[pltpu.VMEM((deep, 2 * hid), BF), pltpu.VMEM((deep, hid), BF)],
        compiler_params=LIMIT,
        name="weight_grads",
    )(line, *factors)


def lay_out(columns, pieces, hid, steps=2):
    width, wide = pieces[0].shape
    n = len(pieces)
    per = wide // (3 * hid)
    total = n * per * hid
    block = width // steps

    def kernel(cols, *refs):
        ins, outs = refs[:n], refs[n:]
        for p in range(n):
            for s in range(per):
                at = pl.multiple_of(cols[p * per + s], hid)
                for m in range(3):
                    o = (s * 3 + m) * hid
                    outs[m][:, pl.ds(at, hid)] = ins[p][:, o : o + hid]

    return pl.pallas_call(
        kernel,
        grid=(steps,),
        out_shape=[jax.ShapeDtypeStruct((width, total), BF)] * 3,
        in_specs=[smem()] + [pl.BlockSpec((block, wide), lambda i: (i, 0))] * n,
        out_specs=[pl.BlockSpec((block, total), lambda i: (i, 0))] * 3,
        compiler_params=LIMIT,
        name="lay_out",
    )(columns, *pieces)


def body(tokens, cotangent, expert_ids, combine_weights, w_gate, w_up, w_down):
    groups = lax.axis_size("ep")
    devices = lax.axis_size("tp")
    chips = devices // 2
    tok_rows, width = tokens.shape
    chosen = expert_ids.shape[1]
    cap = tok_rows * chosen * 5 // (3 * groups)
    rows = groups * cap
    wg, wu, wd = w_gate[0], w_up[0], w_down[0]
    hid = wg.shape[1]
    side = math.isqrt(chips)
    here = lax.axis_index("tp")
    core, cx, cy = here % 2, here // 2 % side, here // (2 * side)
    swap = [(i, i ^ 1) for i in range(devices)]

    def along(v, d, turn=0, other=0):
        pairs = []
        for y in range(side):
            for x in range(side):
                for c in range(2):
                    dx, dy = (d, 0) if c == turn else (0, d)
                    to = ((y + dy) % side * side + (x + dx) % side) * 2 + (c ^ other)
                    pairs.append(((y * side + x) * 2 + c, to))
        return lax.ppermute(v, "tp", pairs)

    def swapped(v):
        return lax.ppermute(v, "tp", swap)

    ids, weights = expert_ids.T, combine_weights.T
    send = dispatch(tokens, cotangent, ids, weights, groups, cap)
    recv = lax.all_to_all(send, "ep", 0, 0, tiled=True)
    piece = (
        jnp.concatenate(
            [recv[:, :cap].reshape(rows, width), recv[:, cap:].reshape(rows, width)], axis=0
        )
    ).T

    place_now = jnp.stack([cx, cy, core])
    steps = (1, 3, 2) if side == 4 else range(1, side)
    order = (0, *steps)

    def line_of(v, turn):
        got = {0: v, **{d: along(v, d, turn) for d in steps}}
        return [got[d] for d in range(side)]

    mine = line_of(jnp.concatenate(line_of(piece, 0)), 1)
    theirs = {d: swapped(mine[d]) for d in order}
    at_once = [(q, j, (mine, theirs)[q][j]) for j in (0,) for q in range(2)]
    later = [(q, j) for j in (1, 3, 2) for q in range(2)]
    ax, ad, ahead, wd_t = early(place_now, at_once, later, wg, wu, wd, width)
    factor, inner, line = late(
        [(mine, theirs)[q][j] for q, j in later], ax, ad, ahead, mine, theirs[0], width
    )
    factors = line_of(factor, 0)

    keep, give = partials(core[None], factor, wg, wu, wd_t, chips, width)
    got = swapped(give)
    inner_got = swapped(inner)
    more = 16
    blocks = add_pair(place_now, keep, got, inner, inner_got, more)

    def exchanged(blocks, turn):
        return [blocks[0]] + [along(blocks[d], d, turn) for d in range(1, side)]

    blocks = exchanged(blocks, 1)
    blocks = add_line(place_now, blocks, width)
    parts = exchanged(blocks, 0)
    back = finish_sum(parts, width, groups)

    grads = weight_grads(line, factors, width)
    pieces = {(0, 0): grads[0]}
    for d in (*steps, 0):
        for q in range(2):
            if (q, d) != (0, 0):
                pieces[q, d] = along(grads[q * side + d], d, 1, q)
    r = jnp.arange(side)
    columns = []
    for q in range(2):
        sender = core ^ q
        for d in range(side):
            fx, fy = (cx - r) % side, (cy - d) % side
            tx, ty = (cx - d) % side, (cy - r) % side
            chip = jnp.where(sender == 0, fy * side + fx, ty * side + tx)
            columns.append((chip * 2 + sender) * hid)
    columns = jnp.concatenate(columns)
    pieces = [pieces[q, d] for q in range(2) for d in range(side)]

    back = lax.all_to_all(back, "ep", 0, 0, tiled=True)
    mixed, grad_tokens, grad_combine = mix(back, ids, weights, width)

    gate_out, up_out, down_out = lay_out(columns, pieces, hid)
    return (
        mixed,
        grad_tokens,
        grad_combine.T,
        gate_out[None],
        up_out[None],
        down_out.T[None],
    )


def solution(mesh):
    return jax.shard_map(
        body,
        mesh=mesh,
        in_specs=(
            P("ep", "tp"),
            P("ep", "tp"),
            P("ep", None),
            P("ep", None),
            P("ep", None, "tp"),
            P("ep", None, "tp"),
            P("ep", "tp", None),
        ),
        out_specs=(
            P("ep", "tp"),
            P("ep", "tp"),
            P("ep", None),
            P("ep", "tp", None),
            P("ep", "tp", None),
            P("ep", None, "tp"),
        ),
        check_vma=False,
    )
```
